32 devices in a mesh: aa: 4 (over x, core), ba: 8 (over z, y).
Axes of the slice: x: 2, y: 2, z: 4, core: 2. Of those that a mesh axis runs over, the one named last changes fastest.
Arguments:
- activations: bfloat16 [1024, 4224], P('aa', 'ba'), may hold values from -6 to 6
- out_grad: bfloat16 [1024, 4096], P('aa', 'ba'), may hold values from -0.1875 to 0.1875
- momentum: float32 [4224, 4096], P('aa', 'ba'), may hold values from -6 to 6
- weight: float32 [4224, 4096], P('aa', 'ba'), may hold values from -6 to 6
- norm_scale: float32 [], replicated, may hold values from 128.99231 to 257.98462
- step_size: float32 [], replicated, may hold values from 0.5 to 2
Outputs:
- new_weight: float32 [4224, 4096], P('aa', 'ba')
- new_momentum: float32 [4224, 4096], P('aa', 'ba')
The draws below stay inside these ranges and needn't reach their ends.
All inputs are finite; a program needn't handle non-finite values.
Results may differ from the reference program's by a relative error of at most 0.00068.
Values may be sent and summed in bfloat16 or wider, within the bound.
A program may use at most 64 MiB of HBM per device.

```python
import math
import jax
import jax.numpy as jnp

ROWS = 4224
COLS = 4096
TOKENS = 1024


def strengthened(result, own_key, source, target, shards_of, factor):
    owner, partner = [(jnp.arange(result.shape[position]) // (result.shape[position] // shards_of)).reshape([-1 if axis == position else 1 for axis in range(result.ndim)]) for position in (source, target)]
    chosen = jax.random.permutation(own_key, shards_of)[partner]
    strong = (owner == chosen) | (owner == (partner + shards_of // 2) % shards_of)
    return jnp.where(strong, factor * result, result)


def steps_of(own_key, extent, cuts, least, high):
    level, own = 1.0, jax.random.fold_in(own_key, 6)
    for position, blocks in cuts:
        heights = jnp.exp(jax.random.uniform(jax.random.fold_in(own, position), (blocks,), jnp.float32, least / len(cuts), high / len(cuts)))
        level = level * jnp.repeat(heights, extent[position] // blocks).reshape([-1 if axis == position else 1 for axis in range(len(extent))])
    return level


def normal_values(own_key, shape, width, most, split=(), kind=jnp.bfloat16):
    array = width * jax.random.normal(own_key, shape, jnp.float32)
    if split:
        array = array * steps_of(own_key, shape, split, -0.22, 0.18)
    return jnp.clip(array, -most, most).astype(kind)


def gaussian_with(own_key, extent, width, limit, pieces, heavy, kind=jnp.bfloat16):
    drawn = width * jax.random.normal(own_key, extent, jnp.float32)
    if pieces:
        drawn = drawn * steps_of(own_key, extent, pieces, -0.22, 0.18)
    return jnp.clip(strengthened(drawn, jax.random.fold_in(own_key, 3), *heavy), -limit, limit).astype(kind)


def setup_inputs(seed: int = 0) -> dict:
    key_of = jax.random.split(jax.random.key(seed), 7)
    return {
        "activations": gaussian_with(key_of[0], (TOKENS, ROWS), 1.0, 6.0, ((0, 4), (1, 8)), (0, 1, 8, 2.0)),
        "out_grad": normal_values(key_of[1], (TOKENS, COLS), (TOKENS ** -0.5), 0.1875, ((0, 4), (1, 8))),
        "momentum": normal_values(key_of[2], (ROWS, COLS), 1.0, 6.0, ((0, 4), (1, 8)), jnp.float32),
        "weight": normal_values(key_of[3], (ROWS, COLS), 1.0, 6.0, ((0, 4), (1, 8)), jnp.float32),
        "norm_scale": jnp.clip(jnp.exp(jax.random.uniform(key_of[4], (), jnp.float32, math.log(128.99231), math.log(257.98462))), 128.99231, 257.98462),
        "step_size": jnp.clip(jnp.exp(jax.random.uniform(key_of[5], (), jnp.float32, math.log(0.5), math.log(2.0))), 0.5, 2.0),
    }


def reference(activations, out_grad, momentum, weight, norm_scale, step_size):
    gradient = jnp.dot(activations.T, out_grad, preferred_element_type=jnp.float32)
    new_momentum = 0.95 * momentum + gradient
    scaled = (new_momentum / norm_scale).astype(jnp.bfloat16)
    gram = jnp.dot(scaled.T, scaled, preferred_element_type=jnp.float32).astype(jnp.bfloat16)
    first_power = jnp.dot(scaled, gram, preferred_element_type=jnp.float32).astype(jnp.bfloat16)
    second_power = jnp.dot(first_power, gram, preferred_element_type=jnp.float32)
    direction = 3.4445 * scaled.astype(jnp.float32) - 4.775 * first_power.astype(jnp.float32) + 2.0315 * second_power
    factor = 0.2 * math.sqrt(max(ROWS, COLS))
    new_weight = weight - step_size * factor * direction
    return (new_weight, new_momentum)
```

```python
import functools
import math

import jax
import jax.numpy as jnp
from jax import lax
from jax.experimental import pallas as pl
from jax.experimental.pallas import tpu as pltpu
from jax.sharding import PartitionSpec as P

ROWS = 4224
COLS = 4096
MESH = pl.DeviceIdType.MESH


def inner_rows(left, right):
    return lax.dot_general(
        left, right, (((0,), (0,)), ((), ())), preferred_element_type=jnp.float32
    )


def powers_kernel(
    n, groups, x_ref, out_ref,
    panel, powers, own_power, gram, parts, from_core, from_chip,
    x_send, x_recv, y_send, y_recv, c_send, c_recv, p_send, p_recv, s_send, s_recv,
):
    rows, width = x_ref.shape
    half, share, middle = rows // 2, width // groups, n // 2
    a, b = lax.axis_index("aa"), lax.axis_index("ba")
    core_mate = a + 1 - 2 * (a % 2)
    chip_mate = (a + 2) % groups

    place = b // 2 + (b % 2) * (n - 1 - 2 * (b // 2))

    def at(position):
        position = (position + n) % n
        column = position // middle
        return 2 * (position + column * (n - 1 - 2 * position)) + column

    neighbours = (at(place + 1), at(place - 1))

    barrier = pltpu.get_barrier_semaphore()
    for d in range(2):
        pl.semaphore_signal(barrier, 1, device_id={"ba": neighbours[d]}, device_id_type=MESH)
    for mate in (core_mate, chip_mate):
        pl.semaphore_signal(barrier, 1, device_id={"aa": mate}, device_id_type=MESH)
    pl.semaphore_wait(barrier, 4)

    def hop(own, held, send, recv, d, s, k):
        target = n - 1 if s == middle else 2 * s - 1 + d
        part = pl.ds(k * half, half)
        source = own.at[part] if s == 1 else held.at[2 * s - 3 + d, part]
        return pltpu.make_async_remote_copy(
            src_ref=source, dst_ref=held.at[target, part],
            send_sem=send.at[d, s - 1, k], recv_sem=recv.at[d, s - 1, k],
            device_id={"ba": neighbours[d]}, device_id_type=MESH,
        )

    def hops(s):
        return [(k, d) for k in range(2) for d in range(2) if s < middle or k == d]

    def ring(own, held, send, recv, use):
        for s in range(1, middle + 1):
            for k, d in hops(s):
                hop(own, held, send, recv, d, s, k).wait_recv()
                if s < middle and (k, d) in hops(s + 1):
                    hop(own, held, send, recv, d, s + 1, k).start()
            use([2 * s - 1, 2 * s] if s < middle else [n - 1])

    def drain(own, held, send, recv):
        for s in range(1, middle + 1):
            for k, d in hops(s):
                hop(own, held, send, recv, d, s, k).wait_send()

    def share_rows(index):
        return pl.ds(pl.multiple_of(index * share, share), share)

    def to_mate(source, target, send, recv, mate):
        return pltpu.make_async_remote_copy(
            src_ref=source, dst_ref=target, send_sem=send, recv_sem=recv,
            device_id={"aa": mate}, device_id_type=MESH,
        )

    def core_copy(e):
        return to_mate(
            parts.at[e, pl.ds(2, 2)], from_core.at[e], c_send.at[e], c_recv.at[e], core_mate
        )

    def chip_copy(e):
        return to_mate(parts.at[e, 1], from_chip.at[e], p_send.at[e], p_recv.at[e], chip_mate)

    def share_copy(e, step):
        mine = gram.at[e, share_rows(chip_mate if step == 2 else a)]
        return to_mate(
            mine, mine, s_send.at[e, step], s_recv.at[e, step],
            chip_mate if step == 0 else core_mate,
        )

    def block(e):
        return x_ref if e == 0 else panel.at[e]

    def gram_partial(e):
        @pl.loop(0, 4)
        def _(r):
            owner = (a + (r // 2) * (1 - 2 * (a % 2)) + 2 * (r % 2)) % groups
            parts[e, r] = inner_rows(block(e)[:, share_rows(owner)], x_ref[...])

        core_copy(e).start()

    def core_sum(e):
        core_copy(e).wait_recv()
        parts[e, 1] = parts[e, 1] + from_core[e, 1]
        chip_copy(e).start()
        parts[e, 0] = parts[e, 0] + from_core[e, 0]

    def gram_share(e):
        chip_copy(e).wait_recv()
        gram[e, share_rows(a)] = (parts[e, 0] + from_chip[e]).astype(jnp.bfloat16)
        share_copy(e, 0).start()
        share_copy(e, 1).start()

    def relay(e):
        share_copy(e, 0).wait_recv()
        share_copy(e, 2).start()

    def gram_ready(e):
        share_copy(e, 1).wait_recv()
        share_copy(e, 2).wait_recv()

    def accumulate(e, source, first, start, count):
        tile = count // 3 if count % 48 == 0 else count

        @pl.loop(0, count // tile)
        def _(t):
            part = pl.ds(pl.multiple_of(start + t * tile, 16), tile)
            term = jnp.dot(source[part, :], gram[e], preferred_element_type=jnp.float32)
            if first:
                out_ref[part, :] = term
            else:
                out_ref[part, :] += term

    for k, d in hops(1):
        hop(x_ref, panel, x_send, x_recv, d, 1, k).start()
    gram_partial(0)
    core_sum(0)
    summed, shared = [0], []

    def use_block(events):
        for e in events:
            gram_partial(e)
        for e in events:
            core_sum(e)
        for e in summed:
            gram_share(e)
        for e in shared:
            relay(e)
        shared[:] = summed
        summed[:] = events

    ring(x_ref, panel, x_send, x_recv, use_block)

    for e in range(n):
        if e == n - 4:
            gram_share(n - 1)
        if e in shared:
            relay(e)
        if e == n - 1:
            relay(e)
        gram_ready(e)
        if e < n - 1:
            accumulate(e, block(e), e == 0, 0, rows)
    for k in range(2):
        accumulate(n - 1, block(n - 1), False, k * half, half)
        part = pl.ds(k * half, half)
        own_power[part, :] = out_ref[part, :].astype(jnp.bfloat16)
        for d in range(2):
            hop(own_power, powers, y_send, y_recv, d, 1, k).start()

    def power_block(e):
        return own_power if e == 0 else powers.at[e]

    accumulate(0, own_power, True, 0, rows)

    def use_power(events):
        for e in events:
            accumulate(e, power_block(e), False, 0, rows)

    ring(own_power, powers, y_send, y_recv, use_power)
    out_ref[...] = (
        3.4445 * x_ref[...].astype(jnp.float32)
        - 4.775 * own_power[...].astype(jnp.float32)
        + 2.0315 * out_ref[...]
    )
    drain(x_ref, panel, x_send, x_recv)
    drain(own_power, powers, y_send, y_recv)
    for e in range(n):
        core_copy(e).wait_send()
        chip_copy(e).wait_send()
        for step in range(3):
            share_copy(e, step).wait_send()


def fused_direction(scaled, n, groups):
    rows, width = scaled.shape
    share = width // groups
    middle = n // 2
    dma = pltpu.SemaphoreType.DMA
    return pl.pallas_call(
        functools.partial(powers_kernel, n, groups),
        out_shape=jax.ShapeDtypeStruct((rows, width), jnp.float32),
        in_specs=[pl.BlockSpec(memory_space=pltpu.VMEM)],
        out_specs=pl.BlockSpec(memory_space=pltpu.VMEM),
        scratch_shapes=[
            pltpu.VMEM((n, rows, width), jnp.bfloat16),
            pltpu.VMEM((n, rows, width), jnp.bfloat16),
            pltpu.VMEM((rows, width), jnp.bfloat16),
            pltpu.VMEM((n, width, width), jnp.bfloat16),
            pltpu.VMEM((n, 4, share, width), jnp.float32),
            pltpu.VMEM((n, 2, share, width), jnp.float32),
            pltpu.VMEM((n, share, width), jnp.float32),
            dma((2, middle, 2)), dma((2, middle, 2)),
            dma((2, middle, 2)), dma((2, middle, 2)),
            dma((n,)), dma((n,)), dma((n,)), dma((n,)),
            dma((n, 3)), dma((n, 3)),
        ],
        compiler_params=pltpu.CompilerParams(
            collective_id=0, has_side_effects=True, vmem_limit_bytes=62 * 1024 * 1024
        ),
        name="powers",
    )(scaled)


def plain_direction(scaled):
    row_panel = lax.all_gather(scaled, "ba", axis=1, tiled=True)
    gram_part = inner_rows(row_panel, scaled)
    width = gram_part.shape[0]
    groups = lax.axis_size("aa")
    padding = (groups - width % groups) % groups
    padded = jnp.pad(gram_part, ((0, padding), (0, 0)))
    share = lax.psum_scatter(padded, "aa", scatter_dimension=0, tiled=True).astype(jnp.bfloat16)
    gram_cols = lax.all_gather(share, "aa", axis=0, tiled=True)[:width]
    first_power = jnp.dot(row_panel, gram_cols, preferred_element_type=jnp.float32).astype(
        jnp.bfloat16
    )
    second_power = jnp.dot(
        lax.all_gather(first_power, "ba", axis=1, tiled=True),
        gram_cols,
        preferred_element_type=jnp.float32,
    )
    return (
        3.4445 * scaled.astype(jnp.float32)
        - 4.775 * first_power.astype(jnp.float32)
        + 2.0315 * second_power
    )


def per_device(activations, out_grad, momentum, weight, norm_scale, step_size):
    features = lax.all_to_all(
        lax.all_gather(activations, "ba", axis=1, tiled=True),
        "aa", split_axis=1, concat_axis=0, tiled=True,
    )
    gradient = inner_rows(features, lax.all_gather(out_grad, "aa", axis=0, tiled=True))
    new_momentum = 0.95 * momentum + gradient
    scaled = (new_momentum / norm_scale).astype(jnp.bfloat16)
    n, groups = lax.axis_size("ba"), lax.axis_size("aa")
    rows, width = scaled.shape
    fits = (
        n % 2 == 0 and n >= 4 and width % 128 == 0
        and width % (16 * groups) == 0 and rows % 32 == 0 and groups == 4
        and (width // groups) % 128 == 0
        and 4 * n * rows * width + 9 * n * width * width + 9 * rows * width < 56 * 2**20
    )
    direction = fused_direction(scaled, n, groups) if fits else plain_direction(scaled)
    factor = 0.2 * math.sqrt(max(ROWS, COLS))
    new_weight = weight - step_size * factor * direction
    return (new_weight, new_momentum)


def solution(mesh):
    placed = (P("aa", "ba"), P("aa", "ba"), P("aa", "ba"), P("aa", "ba"), P(), P())
    return jax.shard_map(
        per_device,
        mesh=mesh,
        in_specs=placed,
        out_specs=(P("aa", "ba"), P("aa", "ba")),
        check_vma=False,
    )
```

```python
import functools
import math

import jax
import jax.numpy as jnp
from jax import lax
from jax.experimental import pallas as pl
from jax.experimental.pallas import tpu as pltpu
from jax.sharding import PartitionSpec as P

ROWS = 4224
COLS = 4096
MESH = pl.DeviceIdType.MESH


def inner_rows(left, right):
    return lax.dot_general(
        left, right, (((0,), (0,)), ((), ())), preferred_element_type=jnp.float32
    )


def powers_kernel(
    n, groups, x_ref, out_ref,
    panel, powers, own_power, gram, parts, from_core, from_chip,
    x_send, x_recv, y_send, y_recv, c_send, c_recv, p_send, p_recv, s_send, s_recv,
):
    rows, width = x_ref.shape
    half, share, middle = rows // 2, width // groups, n // 2
    a, b = lax.axis_index("aa"), lax.axis_index("ba")
    core_mate = a + 1 - 2 * (a % 2)
    chip_mate = (a + 2) % groups

    place = b // 2 + (b % 2) * (n - 1 - 2 * (b // 2))

    def at(position):
        position = (position + n) % n
        column = position // middle
        return 2 * (position + column * (n - 1 - 2 * position)) + column

    neighbours = (at(place + 1), at(place - 1))

    barrier = pltpu.get_barrier_semaphore()
    for d in range(2):
        pl.semaphore_signal(barrier, 1, device_id={"ba": neighbours[d]}, device_id_type=MESH)
    for mate in (core_mate, chip_mate):
        pl.semaphore_signal(barrier, 1, device_id={"aa": mate}, device_id_type=MESH)
    pl.semaphore_wait(barrier, 4)

    def hop(own, held, send, recv, d, s, k):
        target = n - 1 if s == middle else 2 * s - 1 + d
        part = pl.ds(k * half, half)
        source = own.at[part] if s == 1 else held.at[2 * s - 3 + d, part]
        return pltpu.make_async_remote_copy(
            src_ref=source, dst_ref=held.at[target, part],
            send_sem=send.at[d, s - 1, k], recv_sem=recv.at[d, s - 1, k],
            device_id={"ba": neighbours[d]}, device_id_type=MESH,
        )

    def hops(s):
        return [(k, d) for k in range(2) for d in range(2) if s < middle or k == d]

    def ring(own, held, send, recv, use):
        for s in range(1, middle + 1):
            for k, d in hops(s):
                hop(own, held, send, recv, d, s, k).wait_recv()
                if s < middle and (k, d) in hops(s + 1):
                    hop(own, held, send, recv, d, s + 1, k).start()
            use([2 * s - 1, 2 * s] if s < middle else [n - 1])

    def drain(own, held, send, recv):
        for s in range(1, middle + 1):
            for k, d in hops(s):
                hop(own, held, send, recv, d, s, k).wait_send()

    def share_rows(index):
        return pl.ds(pl.multiple_of(index * share, share), share)

    def to_mate(source, target, send, recv, mate):
        return pltpu.make_async_remote_copy(
            src_ref=source, dst_ref=target, send_sem=send, recv_sem=recv,
            device_id={"aa": mate}, device_id_type=MESH,
        )

    def core_copy(e):
        return to_mate(
            parts.at[e, pl.ds(2, 2)], from_core.at[e], c_send.at[e], c_recv.at[e], core_mate
        )

    def chip_copy(e):
        return to_mate(parts.at[e, 1], from_chip.at[e], p_send.at[e], p_recv.at[e], chip_mate)

    def share_copy(e, step):
        mine = gram.at[e, share_rows(chip_mate if step == 2 else a)]
        return to_mate(
            mine, mine, s_send.at[e, step], s_recv.at[e, step],
            chip_mate if step == 0 else core_mate,
        )

    def block(e):
        return x_ref if e == 0 else panel.at[e]

    def gram_partial(e):
        @pl.loop(0, 4)
        def _(r):
            owner = (a + (r // 2) * (1 - 2 * (a % 2)) + 2 * (r % 2)) % groups
            parts[e, r] = inner_rows(block(e)[:, share_rows(owner)], x_ref[...])

        core_copy(e).start()

    def core_sum(e):
        core_copy(e).wait_recv()
        parts[e, 1] = parts[e, 1] + from_core[e, 1]
        chip_copy(e).start()
        parts[e, 0] = parts[e, 0] + from_core[e, 0]

    def gram_share(e):
        chip_copy(e).wait_recv()
        gram[e, share_rows(a)] = (parts[e, 0] + from_chip[e]).astype(jnp.bfloat16)
        share_copy(e, 0).start()
        share_copy(e, 1).start()

    def relay(e):
        share_copy(e, 0).wait_recv()
        share_copy(e, 2).start()

    def gram_ready(e):
        share_copy(e, 1).wait_recv()
        share_copy(e, 2).wait_recv()

    def accumulate(e, source, first, start, count):
        tile = count // 3 if count % 48 == 0 else count

        @pl.loop(0, count // tile)
        def _(t):
            part = pl.ds(pl.multiple_of(start + t * tile, 16), tile)
            term = jnp.dot(source[part, :], gram[e], preferred_element_type=jnp.float32)
            if first:
                out_ref[part, :] = term
            else:
                out_ref[part, :] += term

    for k, d in hops(1):
        hop(x_ref, panel, x_send, x_recv, d, 1, k).start()
    gram_partial(0)
    core_sum(0)
    summed, shared = [0], []

    def use_block(events):
        for e in events:
            gram_partial(e)
        for e in events:
            core_sum(e)
        for e in summed:
            gram_share(e)
        for e in shared:
            relay(e)
        shared[:] = summed
        summed[:] = events

    ring(x_ref, panel, x_send, x_recv, use_block)

    for e in range(n):
        if e == n - 4:
            gram_share(n - 1)
        if e in shared:
            relay(e)
        if e == n - 1:
            relay(e)
        gram_ready(e)
        if e < n - 1:
            accumulate(e, block(e), e == 0, 0, rows)
    for k in range(2):
        accumulate(n - 1, block(n - 1), False, k * half, half)
        part = pl.ds(k * half, half)
        own_power[part, :] = out_ref[part, :].astype(jnp.bfloat16)
        for d in range(2):
            hop(own_power, powers, y_send, y_recv, d, 1, k).start()

    def power_block(e):
        return own_power if e == 0 else powers.at[e]

    accumulate(0, own_power, True, 0, rows)

    def use_power(events):
        for e in events:
            accumulate(e, power_block(e), False, 0, rows)

    ring(own_power, powers, y_send, y_recv, use_power)
    out_ref[...] = (
        3.4445 * x_ref[...].astype(jnp.float32)
        - 4.775 * own_power[...].astype(jnp.float32)
        + 2.0315 * out_ref[...]
    )
    drain(x_ref, panel, x_send, x_recv)
    drain(own_power, powers, y_send, y_recv)
    for e in range(n):
        core_copy(e).wait_send()
        chip_copy(e).wait_send()
        for step in range(3):
            share_copy(e, step).wait_send()


def fused_direction(scaled, n, groups):
    rows, width = scaled.shape
    share = width // groups
    middle = n // 2
    dma = pltpu.SemaphoreType.DMA
    return pl.pallas_call(
        functools.partial(powers_kernel, n, groups),
        out_shape=jax.ShapeDtypeStruct((rows, width), jnp.float32),
        in_specs=[pl.BlockSpec(memory_space=pltpu.VMEM)],
        out_specs=pl.BlockSpec(memory_space=pltpu.VMEM),
        scratch_shapes=[
            pltpu.VMEM((n, rows, width), jnp.bfloat16),
            pltpu.VMEM((n, rows, width), jnp.bfloat16),
            pltpu.VMEM((rows, width), jnp.bfloat16),
            pltpu.VMEM((n, width, width), jnp.bfloat16),
            pltpu.VMEM((n, 4, share, width), jnp.float32),
            pltpu.VMEM((n, 2, share, width), jnp.float32),
            pltpu.VMEM((n, share, width), jnp.float32),
            dma((2, middle, 2)), dma((2, middle, 2)),
            dma((2, middle, 2)), dma((2, middle, 2)),
            dma((n,)), dma((n,)), dma((n,)), dma((n,)),
            dma((n, 3)), dma((n, 3)),
        ],
        compiler_params=pltpu.CompilerParams(
            collective_id=0, has_side_effects=True, vmem_limit_bytes=62 * 1024 * 1024
        ),
        name="powers",
    )(scaled)


def tokens_kernel(
    n, groups, act_ref, grad_ref, act_out, grad_out,
    held, tiles, grads, h_send, h_recv, t_send, t_recv, g_send, g_recv,
):
    middle, half = n // 2, act_ref.shape[0] // 2
    a, b = lax.axis_index("aa"), lax.axis_index("ba")
    place = b // 2 + (b % 2) * (n - 1 - 2 * (b // 2))

    def at(position):
        position = (position + n) % n
        column = position // middle
        return 2 * (position + column * (n - 1 - 2 * position)) + column

    neighbours = (at(place + 1), at(place - 1))
    peers = [(a + r) % groups for r in range(groups)]
    barrier = pltpu.get_barrier_semaphore()
    for d in range(2):
        pl.semaphore_signal(barrier, 1, device_id={"ba": neighbours[d]}, device_id_type=MESH)
    for r in range(1, groups):
        pl.semaphore_signal(barrier, 1, device_id={"aa": peers[r]}, device_id_type=MESH)
    pl.semaphore_wait(barrier, groups + 1)

    def hop(d, s, k):
        target = n - 1 if s == middle else 2 * s - 1 + d
        part = pl.ds(k * half, half)
        source = act_ref.at[part] if s == 1 else held.at[2 * s - 3 + d, part]
        return pltpu.make_async_remote_copy(
            src_ref=source, dst_ref=held.at[target, part],
            send_sem=h_send.at[d, s - 1, k], recv_sem=h_recv.at[d, s - 1, k],
            device_id={"ba": neighbours[d]}, device_id_type=MESH,
        )

    def hops(s):
        return [(k, d) for k in range(2) for d in range(2) if s < middle or k == d]

    def grad_copy(r):
        return pltpu.make_async_remote_copy(
            src_ref=grad_ref, dst_ref=grads.at[a],
            send_sem=g_send.at[r], recv_sem=g_recv.at[r],
            device_id={"aa": peers[r]}, device_id_type=MESH,
        )

    def block(e):
        return act_ref if e == 0 else held.at[e]

    def owner(e):
        if e == 0:
            return b
        if e == n - 1:
            return at(place + middle)
        s = (e + 1) // 2
        return at(place - s) if e % 2 else at(place + s)

    def tile_copy(e):
        index = owner(e)
        return pltpu.make_async_remote_copy(
            src_ref=block(e), dst_ref=tiles.at[index % 2, a],
            send_sem=t_send.at[e], recv_sem=t_recv.at[index % 2, a],
            device_id={"aa": index // 2}, device_id_type=MESH,
        )

    def deliver(e):
        index = owner(e)

        @pl.when(index // 2 != a)
        def _():
            tile_copy(e).start()

        @pl.when(index // 2 == a)
        def _():
            tiles[index % 2, a] = block(e)[...]

    for k, d in hops(1):
        hop(d, 1, k).start()
    deliver(0)
    for r in range(1, groups):
        grad_copy(r).start()
    grads[a] = grad_ref[...]
    for s in range(1, middle + 1):
        for k, d in hops(s):
            hop(d, s, k).wait_recv()
            if s < middle and (k, d) in hops(s + 1):
                hop(d, s + 1, k).start()
        for e in [2 * s - 1, 2 * s] if s < middle else [n - 1]:
            deliver(e)

    for r in range(1, groups):
        grad_copy(r).wait_recv()
        for k in range(2):
            pltpu.make_async_remote_copy(
                src_ref=act_ref, dst_ref=tiles.at[k, peers[r]],
                send_sem=t_send.at[0], recv_sem=t_recv.at[k, peers[r]],
                device_id={"aa": peers[r]}, device_id_type=MESH,
            ).wait_recv()
    act_out[...] = tiles[...]
    grad_out[...] = grads[...]
    for s in range(1, middle + 1):
        for k, d in hops(s):
            hop(d, s, k).wait_send()
    for r in range(1, groups):
        grad_copy(r).wait_send()
    for e in range(n):
        @pl.when(owner(e) // 2 != a)
        def _():
            tile_copy(e).wait_send()


def kernel_gradient(activations, out_grad, n, groups):
    tokens, features = activations.shape
    width = out_grad.shape[1]
    middle = n // 2
    dma = pltpu.SemaphoreType.DMA
    vmem = pl.BlockSpec(memory_space=pltpu.VMEM)
    tiles, grads = pl.pallas_call(
        functools.partial(tokens_kernel, n, groups),
        out_shape=(
            jax.ShapeDtypeStruct((2, groups, tokens, features), jnp.bfloat16),
            jax.ShapeDtypeStruct((groups, tokens, width), jnp.bfloat16),
        ),
        in_specs=[vmem, vmem],
        out_specs=(vmem, vmem),
        scratch_shapes=[
            pltpu.VMEM((n, tokens, features), jnp.bfloat16),
            pltpu.VMEM((2, groups, tokens, features), jnp.bfloat16),
            pltpu.VMEM((groups, tokens, width), jnp.bfloat16),
            dma((2, middle, 2)), dma((2, middle, 2)),
            dma((n,)), dma((2, groups)), dma((groups,)), dma((groups,)),
        ],
        compiler_params=pltpu.CompilerParams(
            collective_id=1, has_side_effects=True, vmem_limit_bytes=48 * 1024 * 1024
        ),
        name="tokens",
    )(activations, out_grad)
    grads = grads.reshape(groups * tokens, width)
    tiles = tiles.reshape(2, groups * tokens, features)
    return jnp.concatenate([inner_rows(tiles[k], grads) for k in range(2)], axis=0)


def plain_gradient(activations, out_grad):
    features = lax.all_to_all(
        lax.all_gather(activations, "ba", axis=1, tiled=True),
        "aa", split_axis=1, concat_axis=0, tiled=True,
    )
    return inner_rows(features, lax.all_gather(out_grad, "aa", axis=0, tiled=True))


def plain_direction(scaled):
    row_panel = lax.all_gather(scaled, "ba", axis=1, tiled=True)
    gram_part = inner_rows(row_panel, scaled)
    width = gram_part.shape[0]
    groups = lax.axis_size("aa")
    padding = (groups - width % groups) % groups
    padded = jnp.pad(gram_part, ((0, padding), (0, 0)))
    share = lax.psum_scatter(padded, "aa", scatter_dimension=0, tiled=True).astype(jnp.bfloat16)
    gram_cols = lax.all_gather(share, "aa", axis=0, tiled=True)[:width]
    first_power = jnp.dot(row_panel, gram_cols, preferred_element_type=jnp.float32).astype(
        jnp.bfloat16
    )
    second_power = jnp.dot(
        lax.all_gather(first_power, "ba", axis=1, tiled=True),
        gram_cols,
        preferred_element_type=jnp.float32,
    )
    return (
        3.4445 * scaled.astype(jnp.float32)
        - 4.775 * first_power.astype(jnp.float32)
        + 2.0315 * second_power
    )


def per_device(activations, out_grad, momentum, weight, norm_scale, step_size):
    n, groups = lax.axis_size("ba"), lax.axis_size("aa")
    rows, width = momentum.shape
    fits = (
        n % 2 == 0 and n >= 4 and width % 128 == 0
        and width % (16 * groups) == 0 and rows % 32 == 0 and groups == 4
        and (width // groups) % 128 == 0
        and 4 * n * rows * width + 9 * n * width * width + 9 * rows * width < 56 * 2**20
    )
    if fits and n == 2 * groups and activations.shape[0] % 32 == 0:
        gradient = kernel_gradient(activations, out_grad, n, groups)
    else:
        gradient = plain_gradient(activations, out_grad)
    new_momentum = 0.95 * momentum + gradient
    scaled = (new_momentum / norm_scale).astype(jnp.bfloat16)
    direction = fused_direction(scaled, n, groups) if fits else plain_direction(scaled)
    factor = 0.2 * math.sqrt(max(ROWS, COLS))
    new_weight = weight - step_size * factor * direction
    return (new_weight, new_momentum)


def solution(mesh):
    placed = (P("aa", "ba"), P("aa", "ba"), P("aa", "ba"), P("aa", "ba"), P(), P())
    return jax.shard_map(
        per_device,
        mesh=mesh,
        in_specs=placed,
        out_specs=(P("aa", "ba"), P("aa", "ba")),
        check_vma=False,
    )
```
